256 devices in a mesh: rows: 64 (over z, y, core), model: 4 (over x).
Axes of the slice: x: 4, y: 4, z: 8, core: 2. Of those that a mesh axis runs over, the one named last changes fastest.
Arguments:
- w_query: float32 [4096, 4096], P('rows', 'model'), may hold values from -0.25 to 0.25
- first_query: float32 [4096, 4096], P('rows', 'model'), may hold values from -6 to 6
- second_query: float32 [4096, 4096], P('rows', 'model'), may hold values from 0.1 to 10
- w_key: float32 [4096, 1024], P('rows', 'model'), may hold values from -0.25 to 0.25
- first_key: float32 [4096, 1024], P('rows', 'model'), may hold values from -6 to 6
- second_key: float32 [4096, 1024], P('rows', 'model'), may hold values from 0.1 to 10
- w_value: float32 [4096, 1024], P('rows', 'model'), may hold values from -0.25 to 0.25
- first_value: float32 [4096, 1024], P('rows', 'model'), may hold values from -6 to 6
- second_value: float32 [4096, 1024], P('rows', 'model'), may hold values from 0.1 to 10
- norm_train: float32 [4096], P(('rows', 'model')), may hold values from 0.25 to 1.75
- norm_step: float32 [4096], P(('rows', 'model')), may hold values from -0.3 to 0.3
Outputs:
- final_query: bfloat16 [4096, 4096], P(None, 'model')
- final_key: bfloat16 [4096, 1024], P(None, 'model')
- final_value: bfloat16 [4096, 1024], P(None, 'model')
- column_query: float32 [4096], P('model')
- column_key: float32 [1024], P('model')
- column_value: float32 [1024], P('model')
- serve_norm: bfloat16 [4096], replicated
- result_query: float32 [4096, 4096], P('rows', 'model')
- result_key: float32 [4096, 1024], P('rows', 'model')
- result_value: float32 [4096, 1024], P('rows', 'model')
The draws below stay inside these ranges and needn't reach their ends.
All inputs are finite; a program needn't handle non-finite values. Where the reference program divides by a largest or mean magnitude, that divisor is 1e-20 or more.
Results may differ from the reference program's by a relative error of at most 0.0004.
Values may be sent and summed in bfloat16 or wider, within the bound.
No kernel may reach another device: no remote copies, remote signals or barrier semaphores. Data moves between devices by JAX's collectives and lax.ppermute only.
A program may use at most 64 MiB of HBM per device.

```python
import math
import jax
import jax.numpy as jnp
from jax import lax

D_MODEL = 4096
Q_DIM = 4096
KV_DIM = 1024


def strengthened(values, key, source, target, shards_of, factor):
    def block_of(dim):
        return (jnp.arange(values.shape[dim]) // (values.shape[dim] // shards_of)).reshape((-1,) + (1,) * (values.ndim - 1 - dim))

    first = jax.random.permutation(key, shards_of)[block_of(target)]
    second = (block_of(target) + shards_of // 2) % shards_of
    return jnp.where((block_of(source) == first) | (block_of(source) == second), factor * values, values)


def steps_of(rng, shape, split, low, largest):
    loudness = 1.0
    for position, parts in split:
        draws = jax.random.uniform(jax.random.fold_in(jax.random.fold_in(rng, 6), position), (parts,), jnp.float32, low / len(split), largest / len(split))
        loudness = loudness * jnp.repeat(jnp.exp(draws), shape[position] // parts).reshape((-1,) + (1,) * (len(shape) - 1 - position))
    return loudness


def gaussian(key, shape, spread, bound, cuts=(), held_as=jnp.bfloat16):
    array = jax.random.normal(key, shape, jnp.float32) * spread
    if len(cuts) > 0:
        array = steps_of(key, shape, cuts, -0.22, 0.18) * array
    return jnp.clip(array, min=-bound, max=bound).astype(held_as)


def noise_with(rng, dims, width, most, cuts, heavy, held_as=jnp.bfloat16):
    array = width * jax.random.normal(rng, dims, jnp.float32)
    if cuts:
        array = array * steps_of(rng, dims, cuts, -0.22, 0.18)
    return jnp.clip(strengthened(array, jax.random.fold_in(rng, 3), *heavy), -most, most).astype(held_as)


def setup_inputs(seed: int = 0) -> dict:
    seeds = jax.random.split(jax.random.key(seed), 12)
    w_query = noise_with(seeds[0], (D_MODEL, Q_DIM), D_MODEL ** -0.5, 0.25, ((0, 64), (1, 4)), (0, 1, 64, 4.0), jnp.float32)
    first_query = gaussian(seeds[1], (D_MODEL, Q_DIM), 1.0, 6.0, ((0, 64), (1, 4)), jnp.float32)
    second_query = jnp.clip(jnp.exp(math.log(10.0) - 4.6051702 * jax.random.uniform(seeds[2], (D_MODEL, Q_DIM), jnp.float32) ** steps_of(seeds[2], (D_MODEL, Q_DIM), ((0, 64), (1, 4)), -0.2, 0.2)), 0.1, 10.0)
    w_key = noise_with(seeds[3], (D_MODEL, KV_DIM), D_MODEL ** -0.5, 0.25, ((0, 64), (1, 4)), (0, 1, 64, 4.0), jnp.float32)
    first_key = gaussian(seeds[4], (D_MODEL, KV_DIM), 1.0, 6.0, ((0, 64), (1, 4)), jnp.float32)
    second_key = jnp.clip(jnp.exp(math.log(10.0) - 4.6051702 * jax.random.uniform(seeds[5], (D_MODEL, KV_DIM), jnp.float32) ** steps_of(seeds[5], (D_MODEL, KV_DIM), ((0, 64), (1, 4)), -0.2, 0.2)), 0.1, 10.0)
    w_value = noise_with(seeds[6], (D_MODEL, KV_DIM), D_MODEL ** -0.5, 0.25, ((0, 64), (1, 4)), (0, 1, 64, 4.0), jnp.float32)
    first_value = gaussian(seeds[7], (D_MODEL, KV_DIM), 1.0, 6.0, ((0, 64), (1, 4)), jnp.float32)
    second_value = jnp.clip(jnp.exp(math.log(10.0) - 4.6051702 * jax.random.uniform(seeds[8], (D_MODEL, KV_DIM), jnp.float32) ** steps_of(seeds[8], (D_MODEL, KV_DIM), ((0, 64), (1, 4)), -0.2, 0.2)), 0.1, 10.0)
    norm_train = jnp.clip(1.0 + 0.15 * jax.random.normal(seeds[9], (D_MODEL,), jnp.float32), 0.25, 1.75)
    norm_step = jnp.clip(jax.random.uniform(seeds[10], (D_MODEL,), jnp.float32, -0.3, 0.3) * steps_of(seeds[10], (D_MODEL,), ((0, 256),), -0.4, 0.0), -0.3, 0.3)
    return dict(w_query=w_query, first_query=first_query, second_query=second_query, w_key=w_key, first_key=first_key, second_key=second_key, w_value=w_value, first_value=first_value, second_value=second_value, norm_train=norm_train, norm_step=norm_step)


learn_rate = 0.01
decay_rate = 0.05
tiny_value = 1e-08

def reference(w_query, first_query, second_query, w_key, first_key, second_key, w_value, first_value, second_value, norm_train, norm_step):
    result_query = w_query - learn_rate * (first_query / (jnp.sqrt(second_query) + tiny_value) + decay_rate * w_query)
    result_key = w_key - learn_rate * (first_key / (jnp.sqrt(second_key) + tiny_value) + decay_rate * w_key)
    result_value = w_value - learn_rate * (first_value / (jnp.sqrt(second_value) + tiny_value) + decay_rate * w_value)
    column_query = lax.optimization_barrier(jnp.sum(jnp.abs(result_query), axis=0)) / D_MODEL
    final_query = (result_query / column_query).astype(jnp.bfloat16)
    column_key = lax.optimization_barrier(jnp.sum(jnp.abs(result_key), axis=0)) / D_MODEL
    final_key = (result_key / column_key).astype(jnp.bfloat16)
    column_value = lax.optimization_barrier(jnp.sum(jnp.abs(result_value), axis=0)) / D_MODEL
    final_value = (result_value / column_value).astype(jnp.bfloat16)
    serve_norm = (norm_train + norm_step).astype(jnp.bfloat16)
    return (final_query, final_key, final_value, column_query, column_key, column_value, serve_norm, result_query, result_key, result_value)
```

```python
import jax
import jax.numpy as jnp
from jax import lax
from jax.sharding import Mesh
from jax.sharding import PartitionSpec as P

ROWS = ("z", "y", "c")
ROWS_X = ("z", "y", "c", "x")

learn_rate = 0.01
decay_rate = 0.05
tiny_value = 1e-08


def step(w, first, second):
    return w - learn_rate * (first / (jnp.sqrt(second) + tiny_value) + decay_rate * w)


def around(value, axis):
    size = lax.axis_size(axis)
    me = lax.axis_index(axis)
    out = jnp.zeros((size, *value.shape), value.dtype)
    out = lax.dynamic_update_index_in_dim(out, value, me, 0)
    for k in range(1, size):
        got = lax.ppermute(value, axis, [(i, (i + k) % size) for i in range(size)])
        out = lax.dynamic_update_index_in_dim(out, got, (me - k) % size, 0)
    return out


def body(wq, fq, sq, wk, fk, sk, wv, fv, sv, norm_train, norm_step):
    d_model = wq.shape[0] * lax.axis_size(ROWS)
    norm = (norm_train + norm_step).astype(jnp.bfloat16)
    norms = around(norm.astype(jnp.float32), "x").ravel()
    rq, rk, rv = step(wq, fq, sq), step(wk, fk, sk), step(wv, fv, sv)
    sums = [jnp.sum(jnp.abs(r), axis=0) for r in (rq, rk, rv)]
    mine = jnp.concatenate(sums + [norms])
    n = lax.axis_size(ROWS)
    everyone = lax.all_to_all(
        jnp.broadcast_to(mine, (n, 1, mine.size)), ROWS, split_axis=0, concat_axis=0, tiled=True
    ).reshape(n, mine.size)
    a = wq.shape[1]
    b = a + wk.shape[1]
    c = b + wv.shape[1]
    total = jnp.sum(everyone[:, :c], axis=0) / d_model
    cq, ck, cv = total[:a], total[a:b], total[b:c]
    serve_norm = everyone[:, c:].reshape(-1).astype(jnp.bfloat16)
    narrow = jnp.concatenate(
        [lax.reduce_precision(r / column, 8, 7) for r, column in ((rq, cq), (rk, ck), (rv, cv))], axis=1
    )
    whole = lax.all_gather(narrow.astype(jnp.float16), ROWS, axis=0, tiled=True)
    final = whole.astype(jnp.bfloat16)
    return final[:, :a], final[:, a:b], final[:, b:], cq, ck, cv, serve_norm, rq, rk, rv


def solution(mesh):
    torus = Mesh(mesh.devices.reshape(8, 4, 2, mesh.shape["model"]), ROWS_X)
    w = P(ROWS, "x")
    return jax.shard_map(
        body,
        mesh=torus,
        in_specs=(w,) * 9 + (P(ROWS_X),) * 2,
        out_specs=(P(None, "x"),) * 3 + (P("x"),) * 3 + (P(),) + (w,) * 3,
        check_vma=False,
    )
```

```python
import jax
import jax.numpy as jnp
from jax import lax
from jax.experimental import pallas as pl
from jax.experimental.pallas import tpu as pltpu
from jax.sharding import Mesh
from jax.sharding import PartitionSpec as P

ROWS = ("z", "y", "c")
ROWS_X = ("z", "y", "c", "x")

learn_rate = 0.01
decay_rate = 0.05
tiny_value = 1e-08


def step(w, first, second):
    return w - learn_rate * (first / (jnp.sqrt(second) + tiny_value) + decay_rate * w)


def moved(value, axis, k):
    n = lax.axis_size(axis)
    return lax.ppermute(value, axis, [(i, (i + k) % n) for i in range(n)])


def around(value, axis):
    size = lax.axis_size(axis)
    me = lax.axis_index(axis)
    out = jnp.zeros((size, *value.shape), value.dtype)
    out = lax.dynamic_update_index_in_dim(out, value, me, 0)
    for k in range(1, size):
        out = lax.dynamic_update_index_in_dim(out, moved(value, axis, k), (me - k) % size, 0)
    return out


def column_means(sums, norms, d_model):
    c = lax.axis_index("c")
    halves = sums.reshape(2, -1)
    half = halves.shape[1]
    keep = jnp.where(c == 0, halves[0], halves[1])
    give = jnp.where(c == 0, halves[1], halves[0])
    mine = jnp.concatenate([keep + moved(give, "c", 1), norms])
    n = lax.axis_size(("z", "y"))
    everyone = lax.all_to_all(
        jnp.broadcast_to(mine, (n, 1, mine.size)), ("z", "y"), split_axis=0, concat_axis=0, tiled=True
    ).reshape(n, mine.size)
    have = jnp.concatenate([jnp.sum(everyone[:, :half], axis=0) / d_model, everyone[:, half:].ravel()])
    other = moved(have, "c", 1)
    pair = [jnp.where(c == 0, have, other), jnp.where(c == 0, other, have)]
    means = jnp.concatenate([p[:half] for p in pair])
    all_norms = jnp.stack([p[half:].reshape(n, -1) for p in pair], axis=1).ravel()
    return means, all_norms


def parted(joined, widths):
    def kernel(joined_ref, *refs):
        outs, sems = refs[: len(widths)], refs[len(widths) :]
        copies, at = [], 0
        for out, sem, wide in zip(outs, sems, widths):
            copies.append(pltpu.make_async_copy(joined_ref.at[:, pl.ds(at, wide)], out, sem))
            copies[-1].start()
            at += wide
        for copy in copies:
            copy.wait()

    return pl.pallas_call(
        kernel,
        out_shape=[jax.ShapeDtypeStruct((joined.shape[0], wide), joined.dtype) for wide in widths],
        in_specs=[pl.BlockSpec(memory_space=pl.ANY)],
        out_specs=[pl.BlockSpec(memory_space=pl.ANY)] * len(widths),
        scratch_shapes=[pltpu.SemaphoreType.DMA] * len(widths),
        compiler_params=pltpu.CompilerParams(vmem_limit_bytes=1 << 20),
        name="parted",
    )(pltpu.with_memory_space_constraint(joined, pltpu.VMEM))


def body(wq, fq, sq, wk, fk, sk, wv, fv, sv, norm_train, norm_step):
    d_model = wq.shape[0] * lax.axis_size(ROWS)
    norm = (norm_train + norm_step).astype(jnp.bfloat16)
    norms = around(norm.astype(jnp.float32), "x").ravel()
    rq, rk, rv = step(wq, fq, sq), step(wk, fk, sk), step(wv, fv, sv)
    sums = jnp.concatenate([jnp.sum(jnp.abs(r), axis=0) for r in (rq, rk, rv)])
    means, all_norms = column_means(sums, norms, d_model)
    serve_norm = all_norms.astype(jnp.bfloat16)
    a = wq.shape[1]
    b = a + wk.shape[1]
    cq, ck, cv = means[:a], means[a:b], means[b:]
    narrow = jnp.concatenate(
        [lax.reduce_precision(r / column, 8, 7) for r, column in ((rq, cq), (rk, ck), (rv, cv))], axis=1
    )
    whole = lax.all_gather(narrow.astype(jnp.float16), ROWS, axis=0, tiled=True)
    final_q, final_k, final_v = parted(whole.astype(jnp.bfloat16), (a, b - a, whole.shape[1] - b))
    return final_q, final_k, final_v, cq, ck, cv, serve_norm, rq, rk, rv


def solution(mesh):
    torus = Mesh(mesh.devices.reshape(8, 4, 2, mesh.shape["model"]), ROWS_X)
    w = P(ROWS, "x")
    return jax.shard_map(
        body,
        mesh=torus,
        in_specs=(w,) * 9 + (P(ROWS_X),) * 2,
        out_specs=(P(None, "x"),) * 3 + (P("x"),) * 3 + (P(),) + (w,) * 3,
        check_vma=False,
    )
```

```python
import jax
import jax.numpy as jnp
from jax import lax
from jax.experimental import pallas as pl
from jax.experimental.pallas import tpu as pltpu
from jax.sharding import Mesh
from jax.sharding import PartitionSpec as P

ROWS = ("z", "y", "c")
ROWS_X = ("z", "y", "c", "x")

learn_rate = 0.01
decay_rate = 0.05
tiny_value = 1e-08
LOTS = 4
COST = 4_000_000


def step(w, first, second):
    return w - learn_rate * (first / (jnp.sqrt(second) + tiny_value) + decay_rate * w)


def moved(value, axis, k):
    n = lax.axis_size(axis)
    return lax.ppermute(value, axis, [(i, (i + k) % n) for i in range(n)])


def column_means(sums, norm, d_model):
    c = lax.axis_index("c")
    halves = sums.reshape(2, -1)
    half = halves.shape[1]
    keep = jnp.where(c == 0, halves[0], halves[1])
    give = jnp.where(c == 0, halves[1], halves[0])
    mine = jnp.concatenate([keep + moved(give, "c", 1), norm])
    n = lax.axis_size(("z", "y"))
    everyone = lax.all_to_all(
        jnp.broadcast_to(mine, (n, 1, mine.size)), ("z", "y"), split_axis=0, concat_axis=0, tiled=True
    ).reshape(n, mine.size)
    have = jnp.concatenate([jnp.sum(everyone[:, :half], axis=0) / d_model, everyone[:, half:].ravel()])
    other = moved(have, "c", 1)
    pair = [jnp.where(c == 0, have, other), jnp.where(c == 0, other, have)]
    means = jnp.concatenate([p[:half] for p in pair])
    norms = jnp.stack([p[half:].reshape(n, -1) for p in pair], axis=1).ravel()
    return means, norms


def placed(finals, parts, core_of, at):
    widths = [f.shape[-1] for f in finals]

    def kernel(*refs):
        ins, refs = refs[: len(parts)], refs[len(parts) :]
        outs, sems = refs[-3 - len(widths) * len(parts) : -len(widths) * len(parts)], refs[-len(widths) * len(parts) :]
        core = core_of(lax.axis_index("c"))
        copies, begin = [], at
        for i, part in enumerate(ins):
            column = 0
            for k, wide in enumerate(widths):
                copies.append(
                    pltpu.make_async_copy(
                        part.at[:, :, pl.ds(column, wide)],
                        outs[k].at[pl.ds(begin, part.shape[0]), core],
                        sems[i * len(widths) + k],
                    )
                )
                copies[-1].start()
                column += wide
            begin += part.shape[0]
        for copy in copies:
            copy.wait()

    have = [] if isinstance(finals[0], jax.ShapeDtypeStruct) else list(finals)
    return pl.pallas_call(
        kernel,
        out_shape=[jax.ShapeDtypeStruct(f.shape, f.dtype) for f in finals],
        in_specs=[pl.BlockSpec(memory_space=pl.ANY)] * (len(parts) + len(have)),
        out_specs=[pl.BlockSpec(memory_space=pl.ANY)] * len(finals),
        scratch_shapes=[pltpu.SemaphoreType.DMA] * (len(widths) * len(parts)),
        input_output_aliases={len(parts) + i: i for i in range(len(have))},
        compiler_params=pltpu.CompilerParams(vmem_limit_bytes=1 << 20),
        cost_estimate=pl.CostEstimate(flops=COST, bytes_accessed=COST, transcendentals=0),
        name="placed",
    )(*[pltpu.with_memory_space_constraint(p, pltpu.VMEM) for p in parts], *have)


def body(wq, fq, sq, wk, fk, sk, wv, fv, sv, norm_train, norm_step):
    d_model = wq.shape[0] * lax.axis_size(ROWS)
    norm = (norm_train + norm_step).astype(jnp.bfloat16)
    xs = lax.axis_size("x")
    slots = jnp.where(jnp.arange(xs)[:, None] == lax.axis_index("x"), norm.astype(jnp.float32)[None], 0.0).ravel()
    rq, rk, rv = step(wq, fq, sq), step(wk, fk, sk), step(wv, fv, sv)
    sums = jnp.concatenate([jnp.sum(jnp.abs(r), axis=0) for r in (rq, rk, rv)])
    means, norms = column_means(sums, slots, d_model)
    a = wq.shape[1]
    b = a + wk.shape[1]
    cq, ck, cv = means[:a], means[a:b], means[b:]
    narrow = jnp.concatenate(
        [lax.reduce_precision(r / column, 8, 7) for r, column in ((rq, cq), (rk, ck), (rv, cv))], axis=1
    )
    rows = wq.shape[0]
    mine = lax.all_gather(narrow.astype(jnp.float16), ("z", "y"), axis=0)
    mine, norms = lax.optimization_barrier((mine, norms.astype(jnp.bfloat16)))
    serve_norm = norms + moved(norms, "x", 1) + moved(norms, "x", 2) + moved(norms, "x", 3)
    blocks = mine.shape[0]
    lot = blocks // LOTS
    theirs = [moved(mine[i : i + lot], "c", 1) for i in range(0, blocks, lot)]
    finals = [jax.ShapeDtypeStruct((blocks, 2, rows, r.shape[1]), jnp.bfloat16) for r in (rq, rk, rv)]
    finals = placed(finals, [mine.astype(jnp.bfloat16)], lambda core: core, 0)
    for i, part in enumerate(theirs):
        finals = placed(finals, [part.astype(jnp.bfloat16)], lambda core: 1 - core, i * lot)
    final_q, final_k, final_v = (f.reshape(d_model, -1) for f in finals)
    return final_q, final_k, final_v, cq, ck, cv, serve_norm, rq, rk, rv


def solution(mesh):
    torus = Mesh(mesh.devices.reshape(8, 4, 2, mesh.shape["model"]), ROWS_X)
    w = P(ROWS, "x")
    return jax.shard_map(
        body,
        mesh=torus,
        in_specs=(w,) * 9 + (P(ROWS_X),) * 2,
        out_specs=(P(None, "x"),) * 3 + (P("x"),) * 3 + (P(),) + (w,) * 3,
        check_vma=False,
    )
```

```python
import jax
import jax.numpy as jnp
from jax import lax
from jax.experimental import pallas as pl
from jax.experimental.pallas import tpu as pltpu
from jax.sharding import Mesh
from jax.sharding import PartitionSpec as P

ROWS = ("z", "y", "c")
ROWS_X = ("z", "y", "c", "x")

learn_rate = 0.01
decay_rate = 0.05
tiny_value = 1e-08


def step(w, first, second):
    return w - learn_rate * (first / (jnp.sqrt(second) + tiny_value) + decay_rate * w)


def moved(value, axis, k):
    n = lax.axis_size(axis)
    return lax.ppermute(value, axis, [(i, (i + k) % n) for i in range(n)])


def column_means(sums, norm, d_model):
    c = lax.axis_index("c")
    halves = sums.reshape(2, -1)
    half = halves.shape[1]
    keep = jnp.where(c == 0, halves[0], halves[1])
    give = jnp.where(c == 0, halves[1], halves[0])
    mine = jnp.concatenate([keep + moved(give, "c", 1), norm])
    n = lax.axis_size(("z", "y"))
    everyone = lax.all_to_all(
        jnp.broadcast_to(mine, (n, 1, mine.size)), ("z", "y"), split_axis=0, concat_axis=0, tiled=True
    ).reshape(n, mine.size)
    have = jnp.concatenate([jnp.sum(everyone[:, :half], axis=0) / d_model, everyone[:, half:].ravel()])
    other = moved(have, "c", 1)
    pair = [jnp.where(c == 0, have, other), jnp.where(c == 0, other, have)]
    means = jnp.concatenate([p[:half] for p in pair])
    norms = jnp.stack([p[half:].reshape(n, -1) for p in pair], axis=1).ravel()
    return means, norms


def parted(joined, widths):
    def kernel(joined_ref, *refs):
        outs, sems = refs[: len(widths)], refs[len(widths) :]
        copies, at = [], 0
        for out, sem, wide in zip(outs, sems, widths):
            copies.append(pltpu.make_async_copy(joined_ref.at[:, pl.ds(at, wide)], out, sem))
            copies[-1].start()
            at += wide
        for copy in copies:
            copy.wait()

    return pl.pallas_call(
        kernel,
        out_shape=[jax.ShapeDtypeStruct((joined.shape[0], wide), joined.dtype) for wide in widths],
        in_specs=[pl.BlockSpec(memory_space=pl.ANY)],
        out_specs=[pl.BlockSpec(memory_space=pl.ANY)] * len(widths),
        scratch_shapes=[pltpu.SemaphoreType.DMA] * len(widths),
        compiler_params=pltpu.CompilerParams(vmem_limit_bytes=1 << 20),
        name="parted",
    )(pltpu.with_memory_space_constraint(joined, pltpu.VMEM))


def body(wq, fq, sq, wk, fk, sk, wv, fv, sv, norm_train, norm_step):
    d_model = wq.shape[0] * lax.axis_size(ROWS)
    norm = (norm_train + norm_step).astype(jnp.bfloat16)
    xs = lax.axis_size("x")
    slots = jnp.where(jnp.arange(xs)[:, None] == lax.axis_index("x"), norm.astype(jnp.float32)[None], 0.0).ravel()
    rq, rk, rv = step(wq, fq, sq), step(wk, fk, sk), step(wv, fv, sv)
    sums = jnp.concatenate([jnp.sum(jnp.abs(r), axis=0) for r in (rq, rk, rv)])
    means, norms = column_means(sums, slots, d_model)
    a = wq.shape[1]
    b = a + wk.shape[1]
    cq, ck, cv = means[:a], means[a:b], means[b:]
    narrow = jnp.concatenate(
        [lax.reduce_precision(r / column, 8, 7) for r, column in ((rq, cq), (rk, ck), (rv, cv))], axis=1
    )
    whole = lax.all_gather(narrow.astype(jnp.float16), ROWS, axis=0, tiled=True)
    norms = norms.astype(jnp.bfloat16)
    norms = norms + moved(norms, "x", 2)
    whole, norms = lax.optimization_barrier((whole, norms))
    serve_norm = norms + moved(norms, "x", 1)
    final_q, final_k, final_v = parted(whole.astype(jnp.bfloat16), (a, b - a, whole.shape[1] - b))
    return final_q, final_k, final_v, cq, ck, cv, serve_norm, rq, rk, rv


def solution(mesh):
    torus = Mesh(mesh.devices.reshape(8, 4, 2, mesh.shape["model"]), ROWS_X)
    w = P(ROWS, "x")
    return jax.shard_map(
        body,
        mesh=torus,
        in_specs=(w,) * 9 + (P(ROWS_X),) * 2,
        out_specs=(P(None, "x"),) * 3 + (P("x"),) * 3 + (P(),) + (w,) * 3,
        check_vma=False,
    )
```

```python
import jax
import jax.numpy as jnp
from jax import lax
from jax.experimental import pallas as pl
from jax.experimental.pallas import tpu as pltpu
from jax.sharding import Mesh
from jax.sharding import PartitionSpec as P

ROWS = ("z", "y", "c")
ROWS_X = ("z", "y", "c", "x")

learn_rate = 0.01
decay_rate = 0.05
tiny_value = 1e-08


def step(w, first, second):
    return w - learn_rate * (first / (jnp.sqrt(second) + tiny_value) + decay_rate * w)


def swapped(value, axis, partner):
    return lax.ppermute(value, axis, [(i, partner(i)) for i in range(lax.axis_size(axis))])


def in_order(c, mine, other):
    return [jnp.where(c == 0, mine, other), jnp.where(c == 0, other, mine)]


def parted(halves, widths):
    chips, _, rows, half = halves.shape

    def kernel(halves_ref, *refs):
        outs, sems = refs[: len(widths)], refs[len(widths) :]
        copies, column = [], 0
        for out, wide in zip(outs, widths):
            done = 0
            while done < wide:
                side, at = divmod(column, half)
                some = min(wide - done, half - at)
                copies.append(
                    pltpu.make_async_copy(
                        halves_ref.at[:, side, :, pl.ds(at, some)],
                        out.at[:, :, pl.ds(done, some)],
                        sems[len(copies)],
                    )
                )
                copies[-1].start()
                done += some
                column += some
        for copy in copies:
            copy.wait()

    return pl.pallas_call(
        kernel,
        out_shape=[jax.ShapeDtypeStruct((chips, rows, wide), halves.dtype) for wide in widths],
        in_specs=[pl.BlockSpec(memory_space=pl.ANY)],
        out_specs=[pl.BlockSpec(memory_space=pl.ANY)] * len(widths),
        scratch_shapes=[pltpu.SemaphoreType.DMA] * (len(widths) + 1),
        compiler_params=pltpu.CompilerParams(vmem_limit_bytes=1 << 20),
        name="parted",
    )(pltpu.with_memory_space_constraint(halves, pltpu.VMEM))


def body(wq, fq, sq, wk, fk, sk, wv, fv, sv, norm_train, norm_step):
    d_model = wq.shape[0] * lax.axis_size(ROWS)
    c = lax.axis_index("c")
    a, b = wq.shape[1], wk.shape[1]
    half = (a + 2 * b) // 2
    rq, rk, rv = step(wq, fq, sq), step(wk, fk, sk), step(wv, fv, sv)

    first, second = rq[:, :half], jnp.concatenate([rq[:, half:], rk, rv], axis=1)
    mine = jnp.where(c == 0, first, second)
    got = swapped(jnp.where(c == 0, second, first), "c", lambda i: 1 - i)
    sums = jnp.sum(jnp.abs(mine), axis=0) + jnp.sum(jnp.abs(got), axis=0)

    norm = (norm_train + norm_step).astype(jnp.bfloat16)
    xs = lax.axis_size("x")
    slots = jnp.where(jnp.arange(xs)[:, None] == lax.axis_index("x"), norm.astype(jnp.float32)[None], 0.0).ravel()
    have = jnp.concatenate([sums, slots])
    chips = lax.axis_size(("z", "y"))
    everyone = lax.all_to_all(
        jnp.broadcast_to(have, (chips, 1, have.size)), ("z", "y"), split_axis=0, concat_axis=0, tiled=True
    ).reshape(chips, have.size)
    mean = jnp.sum(everyone[:, :half], axis=0) / d_model
    means = jnp.concatenate(in_order(c, mean, swapped(mean, "c", lambda i: 1 - i)))
    cq, ck, cv = means[:a], means[a : a + b], means[a + b :]

    rows = jnp.concatenate(in_order(c, mine, got), axis=0)
    narrow = lax.reduce_precision(rows / mean, 8, 7).astype(jnp.float16)
    whole = lax.all_gather(narrow, ROWS, axis=0)

    norms = everyone[:, half:].astype(jnp.bfloat16)
    norms = jnp.where(jnp.arange(2)[:, None] == c, norms[:, None, :], jnp.bfloat16(0)).ravel()
    norms = norms + swapped(norms, "c", lambda i: 1 - i)
    whole, norms = lax.optimization_barrier((whole, norms))
    norms = norms + swapped(norms, "x", lambda i: i ^ 1)
    norms = norms + swapped(norms, "x", lambda i: 3 - i)

    halves = whole.astype(jnp.bfloat16).reshape(chips, 2, *narrow.shape)
    final_q, final_k, final_v = (f.reshape(d_model, -1) for f in parted(halves, (a, b, b)))
    return final_q, final_k, final_v, cq, ck, cv, norms, rq, rk, rv


def solution(mesh):
    torus = Mesh(mesh.devices.reshape(8, 4, 2, mesh.shape["model"]), ROWS_X)
    w = P(ROWS, "x")
    return jax.shard_map(
        body,
        mesh=torus,
        in_specs=(w,) * 9 + (P(ROWS_X),) * 2,
        out_specs=(P(None, "x"),) * 3 + (P("x"),) * 3 + (P(),) + (w,) * 3,
        check_vma=False,
    )
```

```python
import jax
import jax.numpy as jnp
from jax import lax
from jax.experimental import pallas as pl
from jax.experimental.pallas import tpu as pltpu
from jax.sharding import Mesh
from jax.sharding import PartitionSpec as P

ROWS = ("z", "y", "c")
ROWS_X = ("z", "y", "c", "x")

learn_rate = 0.01
decay_rate = 0.05
tiny_value = 1e-08


def step(w, first, second):
    return w - learn_rate * (first / (jnp.sqrt(second) + tiny_value) + decay_rate * w)


def swapped(value, axis, partner):
    return lax.ppermute(value, axis, [(i, partner(i)) for i in range(lax.axis_size(axis))])


def in_order(c, mine, other):
    return [jnp.where(c == 0, mine, other), jnp.where(c == 0, other, mine)]


def parted(halves, means, rows, widths):
    chips, _, tall, half = halves.shape
    tile = (tall - rows, 128)

    def kernel(halves_ref, means_ref, *refs):
        outs, scales, tails, sems = refs[:3], refs[3:6], refs[6], refs[7:]
        copies, column = [], 0

        def copy(source, target):
            copies.append(pltpu.make_async_copy(source, target, sems[len(copies)]))
            copies[-1].start()

        for out, scale, wide in zip(outs, scales, widths):
            copy(means_ref.at[pl.ds(column, wide)], scale)
            done = 0
            while done < wide:
                side, at = divmod(column, half)
                some = min(wide - done, half - at)
                copy(halves_ref.at[:, side, pl.ds(0, rows), pl.ds(at, some)], out.at[:, :, pl.ds(done, some)])
                done += some
                column += some
        copy(halves_ref.at[:, :, pl.ds(rows, tile[0]), pl.ds(0, tile[1])], tails)
        for one in copies:
            one.wait()

    return pl.pallas_call(
        kernel,
        out_shape=[jax.ShapeDtypeStruct((chips, rows, wide), halves.dtype) for wide in widths]
        + [jax.ShapeDtypeStruct((wide,), means.dtype) for wide in widths]
        + [jax.ShapeDtypeStruct((chips, 2, *tile), halves.dtype)],
        in_specs=[pl.BlockSpec(memory_space=pl.ANY)] * 2,
        out_specs=[pl.BlockSpec(memory_space=pl.ANY)] * 7,
        scratch_shapes=[pltpu.SemaphoreType.DMA] * 8,
        compiler_params=pltpu.CompilerParams(vmem_limit_bytes=1 << 20),
        name="parted",
    )(*[pltpu.with_memory_space_constraint(v, pltpu.VMEM) for v in (halves, means)])


def body(wq, fq, sq, wk, fk, sk, wv, fv, sv, norm_train, norm_step):
    d_model = wq.shape[0] * lax.axis_size(ROWS)
    c = lax.axis_index("c")
    a, b = wq.shape[1], wk.shape[1]
    half = (a + 2 * b) // 2
    rq, rk, rv = step(wq, fq, sq), step(wk, fk, sk), step(wv, fv, sv)

    first, second = rq[:, :half], jnp.concatenate([rq[:, half:], rk, rv], axis=1)
    mine = jnp.where(c == 0, first, second)
    got = swapped(jnp.where(c == 0, second, first), "c", lambda i: 1 - i)
    sums = jnp.sum(jnp.abs(mine), axis=0) + jnp.sum(jnp.abs(got), axis=0)

    norm = lax.reduce_precision(norm_train + norm_step, 8, 7)
    sums, norm = lax.optimization_barrier((sums, norm))
    chips = lax.axis_size(("z", "y"))
    everyone = lax.all_to_all(
        jnp.broadcast_to(sums, (chips, 1, half)), ("z", "y"), split_axis=0, concat_axis=0, tiled=True
    ).reshape(chips, half)

    xs = lax.axis_size("x")
    slots = jnp.where(jnp.arange(xs)[:, None] == lax.axis_index("x"), norm[None], 0.0).ravel()
    slots = slots + sum(swapped(slots, "x", lambda i, k=k: (i + k) % xs) for k in range(1, xs))

    mean = jnp.sum(everyone, axis=0) / d_model
    other = swapped(mean, "c", lambda i: 1 - i)
    rows = jnp.concatenate(in_order(c, mine, got), axis=0)
    narrow = lax.reduce_precision(rows / mean, 8, 7)
    tail = jnp.broadcast_to(jnp.pad(slots, (0, half - slots.size)), (8, half))
    narrow = jnp.concatenate([narrow, tail], axis=0).astype(jnp.float16)
    whole = lax.all_gather(narrow, ROWS, axis=0)

    halves = whole.astype(jnp.bfloat16).reshape(chips, 2, *narrow.shape)
    means = jnp.concatenate(in_order(c, mean, other))
    *finals, cq, ck, cv, norms = parted(halves, means, rows.shape[0], (a, b, b))
    final_q, final_k, final_v = (f.reshape(d_model, -1) for f in finals)
    return final_q, final_k, final_v, cq, ck, cv, norms[:, :, 0, : slots.size].ravel(), rq, rk, rv


def solution(mesh):
    torus = Mesh(mesh.devices.reshape(8, 4, 2, mesh.shape["model"]), ROWS_X)
    w = P(ROWS, "x")
    return jax.shard_map(
        body,
        mesh=torus,
        in_specs=(w,) * 9 + (P(ROWS_X),) * 2,
        out_specs=(P(None, "x"),) * 3 + (P("x"),) * 3 + (P(),) + (w,) * 3,
        check_vma=False,
    )
```

```python
import jax
import jax.numpy as jnp
from jax import lax
from jax.experimental import pallas as pl
from jax.experimental.pallas import tpu as pltpu
from jax.sharding import Mesh
from jax.sharding import PartitionSpec as P

ROWS = ("z", "y", "c")
ROWS_X = ("z", "y", "c", "x")

learn_rate = 0.01
decay_rate = 0.05
tiny_value = 1e-08


def step(w, first, second):
    return w - learn_rate * (first / (jnp.sqrt(second) + tiny_value) + decay_rate * w)


def swapped(value, axis, partner):
    return lax.ppermute(value, axis, [(i, partner(i)) for i in range(lax.axis_size(axis))])


def in_order(c, mine, other):
    return [jnp.where(c == 0, mine, other), jnp.where(c == 0, other, mine)]


def parted(halves, means, widths):
    chips, _, rows, half = halves.shape

    def kernel(halves_ref, means_ref, *refs):
        outs, scales, sems = refs[:3], refs[3:6], refs[6:]
        copies, column = [], 0

        def copy(source, target):
            copies.append(pltpu.make_async_copy(source, target, sems[len(copies)]))
            copies[-1].start()

        for out, scale, wide in zip(outs, scales, widths):
            copy(means_ref.at[pl.ds(column, wide)], scale)
            done = 0
            while done < wide:
                side, at = divmod(column, half)
                some = min(wide - done, half - at)
                copy(halves_ref.at[:, side, :, pl.ds(at, some)], out.at[:, :, pl.ds(done, some)])
                done += some
                column += some
        for one in copies:
            one.wait()

    return pl.pallas_call(
        kernel,
        out_shape=[jax.ShapeDtypeStruct((chips, rows, wide), halves.dtype) for wide in widths]
        + [jax.ShapeDtypeStruct((wide,), means.dtype) for wide in widths],
        in_specs=[pl.BlockSpec(memory_space=pl.ANY)] * 2,
        out_specs=[pl.BlockSpec(memory_space=pl.ANY)] * 6,
        scratch_shapes=[pltpu.SemaphoreType.DMA] * 7,
        compiler_params=pltpu.CompilerParams(vmem_limit_bytes=1 << 20),
        name="parted",
    )(*[pltpu.with_memory_space_constraint(v, pltpu.VMEM) for v in (halves, means)])


def body(wq, fq, sq, wk, fk, sk, wv, fv, sv, norm_train, norm_step):
    d_model = wq.shape[0] * lax.axis_size(ROWS)
    c = lax.axis_index("c")
    a, b = wq.shape[1], wk.shape[1]
    half = (a + 2 * b) // 2
    rq, rk, rv = step(wq, fq, sq), step(wk, fk, sk), step(wv, fv, sv)

    first, second = rq[:, :half], jnp.concatenate([rq[:, half:], rk, rv], axis=1)
    mine = jnp.where(c == 0, first, second)
    got = swapped(jnp.where(c == 0, second, first), "c", lambda i: 1 - i)
    sums = jnp.sum(jnp.abs(mine), axis=0) + jnp.sum(jnp.abs(got), axis=0)

    xs = lax.axis_size("x")
    mine_here = (jnp.arange(2)[:, None, None] == c) & (jnp.arange(xs)[:, None] == lax.axis_index("x"))
    slots = jnp.where(mine_here, norm_train + norm_step, 0.0).ravel()
    have = jnp.concatenate([sums, slots])
    chips = lax.axis_size(("z", "y"))
    everyone = lax.all_to_all(
        jnp.broadcast_to(have, (chips, 1, have.size)), ("z", "y"), split_axis=0, concat_axis=0, tiled=True
    ).reshape(chips, have.size)
    mean = jnp.sum(everyone[:, :half], axis=0) / d_model
    other = swapped(mean, "c", lambda i: 1 - i)
    norms = everyone[:, half:].astype(jnp.bfloat16).ravel()
    left = swapped(norms, "x", lambda i: (i + 1) % xs)
    right = swapped(norms, "x", lambda i: (i - 1) % xs)

    rows = jnp.concatenate(in_order(c, mine, got), axis=0)
    narrow = lax.reduce_precision(rows / mean, 8, 7).astype(jnp.float16)
    whole = lax.all_gather(narrow, ROWS, axis=0)

    whole, left, right = lax.optimization_barrier((whole, left, right))
    opposite = swapped(left, "x", lambda i: (i + 1) % xs)
    halves = whole.astype(jnp.bfloat16).reshape(chips, 2, *narrow.shape)
    norms = norms + left + right + opposite
    norms = norms + swapped(norms, "c", lambda i: 1 - i)
    means = jnp.concatenate(in_order(c, mean, other))
    *finals, cq, ck, cv = parted(halves, means, (a, b, b))
    final_q, final_k, final_v = (f.reshape(d_model, -1) for f in finals)
    return final_q, final_k, final_v, cq, ck, cv, norms, rq, rk, rv


def solution(mesh):
    torus = Mesh(mesh.devices.reshape(8, 4, 2, mesh.shape["model"]), ROWS_X)
    w = P(ROWS, "x")
    return jax.shard_map(
        body,
        mesh=torus,
        in_specs=(w,) * 9 + (P(ROWS_X),) * 2,
        out_specs=(P(None, "x"),) * 3 + (P("x"),) * 3 + (P(),) + (w,) * 3,
        check_vma=False,
    )
```

```python
import jax
import jax.numpy as jnp
from jax import lax
from jax.experimental import pallas as pl
from jax.experimental.pallas import tpu as pltpu
from jax.sharding import Mesh
from jax.sharding import PartitionSpec as P

ROWS = ("z", "y", "c")
ROWS_X = ("z", "y", "c", "x")

learn_rate = 0.01
decay_rate = 0.05
tiny_value = 1e-08


def step(w, first, second):
    return w - learn_rate * (first / (jnp.sqrt(second) + tiny_value) + decay_rate * w)


def swapped(value, axis, partner):
    return lax.ppermute(value, axis, [(i, partner(i)) for i in range(lax.axis_size(axis))])


def in_order(c, mine, other):
    return [jnp.where(c == 0, mine, other), jnp.where(c == 0, other, mine)]


def parted(halves, means, norms, widths):
    chips, _, rows, half = halves.shape
    half //= 2

    def kernel(halves_ref, means_ref, norms_ref, *refs):
        outs, scales, whole_norm, sems = refs[:3], refs[3:6], refs[6], refs[7:]
        copies, column = [], 0

        def copy(source, target):
            copies.append(pltpu.make_async_copy(source, target, sems[len(copies)]))
            copies[-1].start()

        for out, scale, wide in zip(outs, scales, widths):
            copy(means_ref.at[pl.ds(column, wide)], scale)
            done = 0
            while done < wide:
                side, at = divmod(column, half)
                some = min(wide - done, half - at)
                for core in range(2):
                    source = halves_ref.at[:, side, :, pl.ds(core * half + at, some)]
                    copy(source, out.at[:, core, :, pl.ds(done, some)])
                done += some
                column += some
        copy(norms_ref, whole_norm)
        for one in copies:
            one.wait()

    return pl.pallas_call(
        kernel,
        out_shape=[jax.ShapeDtypeStruct((chips, 2, rows, wide), halves.dtype) for wide in widths]
        + [jax.ShapeDtypeStruct((wide,), means.dtype) for wide in widths]
        + [jax.ShapeDtypeStruct(norms.shape, norms.dtype)],
        in_specs=[pl.BlockSpec(memory_space=pl.ANY)] * 3,
        out_specs=[pl.BlockSpec(memory_space=pl.ANY)] * 7,
        scratch_shapes=[pltpu.SemaphoreType.DMA] * 12,
        compiler_params=pltpu.CompilerParams(vmem_limit_bytes=1 << 20),
        name="parted",
    )(*[pltpu.with_memory_space_constraint(v, pltpu.VMEM) for v in (halves, means, norms)])


def body(wq, fq, sq, wk, fk, sk, wv, fv, sv, norm_train, norm_step):
    d_model = wq.shape[0] * lax.axis_size(ROWS)
    c = lax.axis_index("c")
    a, b = wq.shape[1], wk.shape[1]
    half = (a + 2 * b) // 2

    xs = lax.axis_size("x")
    mine_here = (jnp.arange(2)[:, None, None] == c) & (jnp.arange(xs)[:, None] == lax.axis_index("x"))
    slots = jnp.where(mine_here, norm_train + norm_step, 0.0).ravel()
    near = swapped(slots, "x", lambda i: i ^ 1)
    slots = slots + near
    far = swapped(slots, "x", lambda i: xs - 1 - i)
    slots = slots + far

    rq = step(wq, fq, sq)
    rk, rv = step(wk, fk, sk), step(wv, fv, sv)

    first, second = rq[:, :half], jnp.concatenate([rq[:, half:], rk, rv], axis=1)
    mine = jnp.where(c == 0, first, second)
    got = swapped(jnp.where(c == 0, second, first), "c", lambda i: 1 - i)
    sums = jnp.sum(jnp.abs(mine), axis=0) + jnp.sum(jnp.abs(got), axis=0)

    have = jnp.concatenate([sums, slots])
    chips = lax.axis_size(("z", "y"))
    everyone = lax.all_to_all(
        jnp.broadcast_to(have, (chips, 1, have.size)), ("z", "y"), split_axis=0, concat_axis=0, tiled=True
    ).reshape(chips, have.size)
    mean = jnp.sum(everyone[:, :half], axis=0) / d_model
    other = swapped(mean, "c", lambda i: 1 - i)
    norms = everyone[:, half:].astype(jnp.bfloat16).ravel()
    other_norms = swapped(norms, "c", lambda i: 1 - i)

    rows = jnp.concatenate(in_order(c, mine, got), axis=1)
    narrow = lax.reduce_precision(rows / jnp.concatenate([mean, mean]), 8, 7).astype(jnp.float16)
    whole = lax.all_gather(narrow, ROWS, axis=0)

    halves = whole.astype(jnp.bfloat16).reshape(chips, 2, *narrow.shape)
    means = jnp.concatenate(in_order(c, mean, other))
    *finals, cq, ck, cv, norms = parted(halves, means, norms + other_norms, (a, b, b))
    final_q, final_k, final_v = (f.reshape(d_model, -1) for f in finals)
    return final_q, final_k, final_v, cq, ck, cv, norms, rq, rk, rv


def solution(mesh):
    torus = Mesh(mesh.devices.reshape(8, 4, 2, mesh.shape["model"]), ROWS_X)
    w = P(ROWS, "x")
    return jax.shard_map(
        body,
        mesh=torus,
        in_specs=(w,) * 9 + (P(ROWS_X),) * 2,
        out_specs=(P(None, "x"),) * 3 + (P("x"),) * 3 + (P(),) + (w,) * 3,
        check_vma=False,
    )
```

```python
import jax
import jax.numpy as jnp
from jax import lax
from jax.experimental import pallas as pl
from jax.experimental.pallas import tpu as pltpu
from jax.sharding import Mesh
from jax.sharding import PartitionSpec as P

ROWS = ("z", "y", "c")
ROWS_X = ("z", "y", "c", "x")

learn_rate = 0.01
decay_rate = 0.05
tiny_value = 1e-08


def step(w, first, second):
    return w - learn_rate * (first / (jnp.sqrt(second) + tiny_value) + decay_rate * w)


def swapped(value, axis, partner):
    return lax.ppermute(value, axis, [(i, partner(i)) for i in range(lax.axis_size(axis))])


def in_order(c, mine, other):
    return [jnp.where(c == 0, mine, other), jnp.where(c == 0, other, mine)]


def parted(halves, means, rows, widths):
    chips, _, tall, half = halves.shape
    tile = (tall - rows, 128)

    def kernel(halves_ref, means_ref, *refs):
        outs, scales, tails, sems = refs[:3], refs[3:6], refs[6], refs[7:]
        copies, column = [], 0

        def copy(source, target):
            copies.append(pltpu.make_async_copy(source, target, sems[len(copies)]))
            copies[-1].start()

        for out, scale, wide in zip(outs, scales, widths):
            copy(means_ref.at[pl.ds(column, wide)], scale)
            done = 0
            while done < wide:
                side, at = divmod(column, half)
                some = min(wide - done, half - at)
                copy(halves_ref.at[:, side, pl.ds(0, rows), pl.ds(at, some)], out.at[:, :, pl.ds(done, some)])
                done += some
                column += some
        copy(halves_ref.at[:, :, pl.ds(rows, tile[0]), pl.ds(0, tile[1])], tails)
        for one in copies:
            one.wait()

    return pl.pallas_call(
        kernel,
        out_shape=[jax.ShapeDtypeStruct((chips, rows, wide), halves.dtype) for wide in widths]
        + [jax.ShapeDtypeStruct((wide,), means.dtype) for wide in widths]
        + [jax.ShapeDtypeStruct((chips, 2, *tile), halves.dtype)],
        in_specs=[pl.BlockSpec(memory_space=pl.ANY)] * 2,
        out_specs=[pl.BlockSpec(memory_space=pl.ANY)] * 7,
        scratch_shapes=[pltpu.SemaphoreType.DMA] * 8,
        compiler_params=pltpu.CompilerParams(vmem_limit_bytes=1 << 20),
        name="parted",
    )(*[pltpu.with_memory_space_constraint(v, pltpu.VMEM) for v in (halves, means)])


def body(wq, fq, sq, wk, fk, sk, wv, fv, sv, norm_train, norm_step):
    d_model = wq.shape[0] * lax.axis_size(ROWS)
    c = lax.axis_index("c")
    a, b = wq.shape[1], wk.shape[1]
    half = (a + 2 * b) // 2
    rq, rk, rv = step(wq, fq, sq), step(wk, fk, sk), step(wv, fv, sv)

    first, second = rq[:, :half], jnp.concatenate([rq[:, half:], rk, rv], axis=1)
    mine = jnp.where(c == 0, first, second)
    got = swapped(jnp.where(c == 0, second, first), "c", lambda i: 1 - i)
    sums = jnp.sum(jnp.abs(mine), axis=0) + jnp.sum(jnp.abs(got), axis=0)

    norm = lax.reduce_precision(norm_train + norm_step, 8, 7)
    sums, norm = lax.optimization_barrier((sums, norm))
    chips = lax.axis_size(("z", "y"))
    everyone = lax.all_to_all(
        jnp.broadcast_to(sums, (chips, 1, half)), ("z", "y"), split_axis=0, concat_axis=0, tiled=True
    ).reshape(chips, half)

    xs = lax.axis_size("x")
    slots = jnp.where(jnp.arange(xs)[:, None] == lax.axis_index("x"), norm[None], 0.0).ravel()
    opposite = swapped(slots, "x", lambda i: (i + 2) % xs)
    slots = slots + swapped(slots, "x", lambda i: (i + 1) % xs) + swapped(slots, "x", lambda i: (i - 1) % xs)
    slots = slots + opposite

    mean = jnp.sum(everyone, axis=0) / d_model
    other = swapped(mean, "c", lambda i: 1 - i)
    rows = jnp.concatenate(in_order(c, mine, got), axis=0)
    narrow = lax.reduce_precision(rows / mean, 8, 7)
    tail = jnp.broadcast_to(jnp.pad(slots, (0, half - slots.size)), (8, half))
    narrow = jnp.concatenate([narrow, tail], axis=0).astype(jnp.float16)
    whole = lax.all_gather(narrow, ROWS, axis=0, tiled=True)

    halves = whole.astype(jnp.bfloat16).reshape(chips, 2, *narrow.shape)
    means = jnp.concatenate(in_order(c, mean, other))
    *finals, cq, ck, cv, norms = parted(halves, means, rows.shape[0], (a, b, b))
    final_q, final_k, final_v = (f.reshape(d_model, -1) for f in finals)
    return final_q, final_k, final_v, cq, ck, cv, norms[:, :, 0, : slots.size].ravel(), rq, rk, rv


def solution(mesh):
    torus = Mesh(mesh.devices.reshape(8, 4, 2, mesh.shape["model"]), ROWS_X)
    w = P(ROWS, "x")
    return jax.shard_map(
        body,
        mesh=torus,
        in_specs=(w,) * 9 + (P(ROWS_X),) * 2,
        out_specs=(P(None, "x"),) * 3 + (P("x"),) * 3 + (P(),) + (w,) * 3,
        check_vma=False,
    )
```

```python
import jax
import jax.numpy as jnp
from jax import lax
from jax.experimental import pallas as pl
from jax.experimental.pallas import tpu as pltpu
from jax.sharding import Mesh
from jax.sharding import PartitionSpec as P

ROWS = ("z", "y", "c")
ROWS_X = ("z", "y", "c", "x")

learn_rate = 0.01
decay_rate = 0.05
tiny_value = 1e-08


def step(w, first, second):
    return w - learn_rate * (first / (jnp.sqrt(second) + tiny_value) + decay_rate * w)


def moved(value, axis, k):
    n = lax.axis_size(axis)
    return lax.ppermute(value, axis, [(i, (i + k) % n) for i in range(n)])


def column_means(sums, norm, d_model):
    c = lax.axis_index("c")
    halves = sums.reshape(2, -1)
    half = halves.shape[1]
    keep = jnp.where(c == 0, halves[0], halves[1])
    give = jnp.where(c == 0, halves[1], halves[0])
    mine = jnp.concatenate([keep + moved(give, "c", 1), norm])
    n = lax.axis_size(("z", "y"))
    everyone = lax.all_to_all(
        jnp.broadcast_to(mine, (n, 1, mine.size)), ("z", "y"), split_axis=0, concat_axis=0, tiled=True
    ).reshape(n, mine.size)
    have = jnp.sum(everyone[:, :half], axis=0) / d_model
    other = moved(have, "c", 1)
    means = jnp.concatenate([jnp.where(c == 0, have, other), jnp.where(c == 0, other, have)])
    return means, everyone[:, half:].astype(jnp.bfloat16).ravel()


def parted(joined, widths):
    def kernel(joined_ref, *refs):
        outs, sems = refs[: len(widths)], refs[len(widths) :]
        copies, at = [], 0
        for out, sem, wide in zip(outs, sems, widths):
            copies.append(pltpu.make_async_copy(joined_ref.at[:, pl.ds(at, wide)], out, sem))
            copies[-1].start()
            at += wide
        for copy in copies:
            copy.wait()

    return pl.pallas_call(
        kernel,
        out_shape=[jax.ShapeDtypeStruct((joined.shape[0], wide), joined.dtype) for wide in widths],
        in_specs=[pl.BlockSpec(memory_space=pl.ANY)],
        out_specs=[pl.BlockSpec(memory_space=pl.ANY)] * len(widths),
        scratch_shapes=[pltpu.SemaphoreType.DMA] * len(widths),
        compiler_params=pltpu.CompilerParams(vmem_limit_bytes=1 << 20),
        name="parted",
    )(pltpu.with_memory_space_constraint(joined, pltpu.VMEM))


def body(wq, fq, sq, wk, fk, sk, wv, fv, sv, norm_train, norm_step):
    d_model = wq.shape[0] * lax.axis_size(ROWS)
    c, x = lax.axis_index("c"), lax.axis_index("x")
    mine_here = (jnp.arange(2)[:, None, None] == c) & (jnp.arange(lax.axis_size("x"))[:, None] == x)
    slots = jnp.where(mine_here, norm_train + norm_step, 0.0).ravel()
    rq, rk, rv = step(wq, fq, sq), step(wk, fk, sk), step(wv, fv, sv)
    sums = jnp.concatenate([jnp.sum(jnp.abs(r), axis=0) for r in (rq, rk, rv)])
    means, norms = column_means(sums, slots, d_model)
    a = wq.shape[1]
    b = a + wk.shape[1]
    cq, ck, cv = means[:a], means[a:b], means[b:]
    narrow = jnp.concatenate(
        [lax.reduce_precision(r / column, 8, 7) for r, column in ((rq, cq), (rk, ck), (rv, cv))], axis=1
    )
    whole = lax.all_gather(narrow.astype(jnp.float16), ROWS, axis=0, tiled=True)
    opposite = moved(norms, "x", 2)
    whole, opposite = lax.optimization_barrier((whole, opposite))
    norms = norms + opposite
    partner = moved(norms, "c", 1)
    norms = norms + partner
    joined = whole.astype(jnp.bfloat16)
    serve_norm = norms + moved(norms, "x", 1)
    final_q, final_k, final_v = parted(joined, (a, b - a, whole.shape[1] - b))
    return final_q, final_k, final_v, cq, ck, cv, serve_norm, rq, rk, rv


def solution(mesh):
    torus = Mesh(mesh.devices.reshape(8, 4, 2, mesh.shape["model"]), ROWS_X)
    w = P(ROWS, "x")
    return jax.shard_map(
        body,
        mesh=torus,
        in_specs=(w,) * 9 + (P(ROWS_X),) * 2,
        out_specs=(P(None, "x"),) * 3 + (P("x"),) * 3 + (P(),) + (w,) * 3,
        check_vma=False,
    )
```
